32 devices in a mesh: gx: 4 (over x, core), gy: 4 (over z), gz: 2 (over y).
Axes of the slice: x: 2, y: 2, z: 4, core: 2. Of those that a mesh axis runs over, the one named last changes fastest.
Arguments:
- density: float32 [32, 64, 256], P('gx', 'gy', 'gz'), may hold values from 0.1 to 10
- x_faces: float32 [2, 64, 256], P(None, 'gy', 'gz'), may hold values from -6 to 6
- y_faces: float32 [2, 32, 256], P(None, 'gx', 'gz'), may hold values from -6 to 6
- z_faces: float32 [2, 32, 64], P(None, 'gx', 'gy'), may hold values from -6 to 6
Outputs:
- solution_field: float32 [32, 64, 256], P('gx', 'gy', 'gz')
- residual: float32 [32, 64, 256], P('gx', 'gy', 'gz')
The draws below stay inside these ranges and needn't reach their ends.
All inputs are finite; a program needn't handle non-finite values.
Results may differ from the reference program's by a relative error of at most 0.0003.
Values sent between devices are 32-bit elements; how exact they have to be, the bound alone decides.
A program may use at most 64 MiB of HBM per device.

```python
import jax
import jax.numpy as jnp

ITERS = 2
LEVELS = 3
COARSE_SWEEPS = 3
NX = 32
NY = 64
NZ = 256


def draw_density(key, part):
    rough_key = jax.random.fold_in(key, 11)
    x_frac = jnp.arange(NX, dtype=jnp.float32) / NX
    rough = jnp.exp(jax.random.uniform(rough_key, (NX, NY, NZ), jnp.float32, jnp.log(0.5), jnp.log(2.0)))
    profile = jnp.exp(jnp.log(3.0) * x_frac)[:, None, None]
    return (rough * profile).astype(jnp.float32)


def shard_levels(stream_key, dims, pieces, least, largest):
    def one(axis_at, blocks):
        heights = jax.random.uniform(jax.random.fold_in(jax.random.fold_in(stream_key, 6), axis_at), (blocks,), jnp.float32, least / len(pieces), largest / len(pieces))
        return jnp.repeat(jnp.exp(heights), dims[axis_at] // blocks).reshape((-1,) + (1,) * (len(dims) - axis_at - 1))

    level = one(*pieces[0])
    for cut in pieces[1:]:
        level = level * one(*cut)
    return level


def bell_draw(stream_key, dims, width, most, cuts=(), kind=jnp.bfloat16):
    gain = shard_levels(stream_key, dims, cuts, -0.22, 0.18) if cuts else 1.0
    array = jax.random.normal(stream_key, dims, jnp.float32) * width * gain
    return jnp.minimum(jnp.maximum(array, -most), most).astype(kind)


def setup_inputs(seed: int = 0) -> dict:
    key_list = jax.random.split(jax.random.key(seed), 5)
    density = draw_density(jax.random.fold_in(key_list[4], 71), 0)
    x_faces = bell_draw(key_list[1], (2, NY, NZ), 1.0, 6.0, ((1, 4), (2, 2)), jnp.float32)
    y_faces = bell_draw(key_list[2], (2, NX, NZ), 1.0, 6.0, ((1, 4), (2, 2)), jnp.float32)
    z_faces = bell_draw(key_list[3], (2, NX, NY), 1.0, 6.0, ((1, 4), (2, 4)), jnp.float32)
    return dict(density=density, x_faces=x_faces, y_faces=y_faces, z_faces=z_faces)


relax_rate = 1.0 / 9.0
coupling = 0.5


def beside_sum(padded):
    beside = padded[2:, 1:-1, 1:-1] + padded[:-2, 1:-1, 1:-1]
    beside = beside + padded[1:-1, 2:, 1:-1] + padded[1:-1, :-2, 1:-1]
    beside = beside + padded[1:-1, 1:-1, 2:] + padded[1:-1, 1:-1, :-2]
    return beside


def operate(field):
    return 6.0 * field - beside_sum(jnp.pad(field, 1))


def restrict(field):
    sx, sy, sz = field.shape
    return 0.5 * jnp.sum(field.reshape(sx // 2, 2, sy // 2, 2, sz // 2, 2), axis=(1, 3, 5))


def prolong(field):
    sx, sy, sz = field.shape
    spread = jnp.broadcast_to(field[:, None, :, None, :, None], (sx, 2, sy, 2, sz, 2))
    return spread.reshape(2 * sx, 2 * sy, 2 * sz)


def cycle(right_side, level_idx):
    approx = relax_rate * right_side
    if level_idx == LEVELS - 1:
        for sweep_idx in range(COARSE_SWEEPS - 1):
            approx = approx + relax_rate * (right_side - operate(approx))
        return approx
    defect = right_side - operate(approx)
    approx = approx + prolong(cycle(restrict(defect), level_idx + 1))
    return approx + relax_rate * (right_side - operate(approx))


def reference(density, x_faces, y_faces, z_faces):
    right_side = -coupling * density
    right_side = right_side.at[0].add(x_faces[0])
    right_side = right_side.at[-1].add(x_faces[1])
    right_side = right_side.at[:, 0].add(y_faces[0])
    right_side = right_side.at[:, -1].add(y_faces[1])
    right_side = right_side.at[:, :, 0].add(z_faces[0])
    right_side = right_side.at[:, :, -1].add(z_faces[1])
    solution_field = jnp.zeros_like(right_side)
    residual = right_side
    precond = cycle(residual, 0)
    direction = precond
    gamma_now = jnp.sum(residual * precond)
    for iteration in range(ITERS):
        image = operate(direction)
        step_size = gamma_now / jnp.sum(direction * image)
        solution_field = solution_field + step_size * direction
        residual = residual - step_size * image
        if iteration + 1 < ITERS:
            precond = cycle(residual, 0)
            gamma_next = jnp.sum(residual * precond)
            direction = precond + (gamma_next / gamma_now) * direction
            gamma_now = gamma_next
    return solution_field, residual
```

```python
import functools

import jax
import jax.numpy as jnp
from jax import lax
from jax.experimental import pallas as pl
from jax.experimental.pallas import tpu as pltpu
from jax.sharding import PartitionSpec as P

W = 1.0 / 9.0
COUPLING = 0.5
MESH = pl.DeviceIdType.MESH
REACH = 7


def lane_of(shape):
    return lax.broadcasted_iota(jnp.int32, shape, len(shape) - 1)


def roll(x, shift, axis):
    return pltpu.roll(x, shift % x.shape[axis], axis)


def kernel(
    ns, bx, by, bz, kx, ky,
    den, xf, yf, zf, sol, res,
    fld, ysrc, yrec, zsrc, zrec, tmp, prol, dsrc, win, sums,
    fsend, frecv, dsend, drecv, ssend, srecv, *rest,
):
    nx, ny, nz = ns
    gx, gy, gz = (lax.axis_index(a) for a in ("gx", "gy", "gz"))
    hx, hy, hz = bx // 2, by // 2, bz // 2
    me = (gx * ny + gy) * nz + gz
    total = nx * ny * nz
    f32 = jnp.float32

    fld[...] = jnp.zeros_like(fld)
    yrec[...] = jnp.zeros_like(yrec)
    zrec[...] = jnp.zeros_like(zrec)
    win[...] = jnp.zeros_like(win)

    barrier = pltpu.get_barrier_semaphore()

    def coords(flat):
        return (flat // (ny * nz), lax.rem(flat // nz, ny), lax.rem(flat, nz))

    def greet(step, c):
        other = lax.rem(me + step, total)
        pl.semaphore_signal(barrier, inc=1, device_id=coords(other), device_id_type=MESH)
        return c

    lax.fori_loop(1, total, greet, 0)

    lane = lane_of((by, bz))
    eye = lax.broadcasted_iota(jnp.int32, (by, by), 0) == lax.broadcasted_iota(jnp.int32, (by, by), 1)
    row = lax.broadcasted_iota(jnp.int32, (by, bz), 0)
    planes = []
    for p in range(bx):
        r = -COUPLING * den[p]
        if p == 0:
            r = r + jnp.where(gx == 0, xf[0], 0.0)
        if p == bx - 1:
            r = r + jnp.where(gx == nx - 1, xf[1], 0.0)
        r = r + jnp.where((row == 0) & (gy == 0), yf[0, p : p + 1, :], 0.0)
        r = r + jnp.where((row == by - 1) & (gy == ny - 1), yf[1, p : p + 1, :], 0.0)
        for side, (at, edge) in enumerate(((0, 0), (bz - 1, nz - 1))):
            col = jnp.sum(jnp.where(eye, zf[side, p : p + 1, :], 0.0), axis=1, keepdims=True)
            r = r + jnp.where((lane == at) & (gz == edge), col, 0.0)
        planes.append(r)
    r0 = jnp.stack(planes)

    pl.semaphore_wait(barrier, total - 1)

    def pack(field, at, rep):
        out = jnp.zeros((by, bz), f32)
        for p in range(bx):
            out = jnp.where(lane == p, roll(field[p // rep], p - at, 1), out)
        return out

    def faces(k, do):
        def one(s, src, dst, dev, there, back):
            if do == "start":
                @pl.when(there)
                def _():
                    pltpu.make_async_remote_copy(
                        src, dst, fsend.at[k, s], frecv.at[k, s], device_id=dev, device_id_type=MESH
                    ).start()
            else:
                @pl.when(there)
                def _():
                    pltpu.make_async_remote_copy(
                        src, dst, fsend.at[k, s], frecv.at[k, s], device_id=dev, device_id_type=MESH
                    ).wait_send()

                @pl.when(back)
                def _():
                    pltpu.make_async_remote_copy(
                        src, dst, fsend.at[k, s], frecv.at[k, s], device_id=dev, device_id_type=MESH
                    ).wait_recv()

        own = pl.ds(8, by)
        xl, xr, yl, yr, zl, zr = gx > 0, gx < nx - 1, gy > 0, gy < ny - 1, gz > 0, gz < nz - 1
        one(0, fld.at[k, bx, own], fld.at[k, 0, own], (gx + 1, gy, gz), xr, xl)
        one(1, fld.at[k, 1, own], fld.at[k, bx + 1, own], (gx - 1, gy, gz), xl, xr)
        one(2, ysrc.at[k, 1], yrec.at[k, 0], (gx, gy + 1, gz), yr, yl)
        one(3, ysrc.at[k, 0], yrec.at[k, 1], (gx, gy - 1, gz), yl, yr)
        one(4, zsrc.at[k, 1], zrec.at[k, 0], (gx, gy, gz + 1), zr, zl)
        one(5, zsrc.at[k, 0], zrec.at[k, 1], (gx, gy, gz - 1), zl, zr)

    def exchange(k, value):
        fld[k, 1 : bx + 1, 8 : 8 + by, :] = value
        for p in range(bx):
            ysrc[k, 0, p : p + 1, :] = value[p, 0:1, :]
            ysrc[k, 1, p : p + 1, :] = value[p, by - 1 : by, :]
        zsrc[k, 0] = pack(value, 0, 1)
        zsrc[k, 1] = pack(value, bz - 1, 1)
        faces(k, "start")
        faces(k, "wait")
        for p in range(bx):
            fld[k, p + 1, 7:8, :] = yrec[k, 0, p : p + 1, :]
            fld[k, p + 1, 8 + by : 9 + by, :] = yrec[k, 1, p : p + 1, :]

    def operate(ref, zl, zr):
        out = []
        for p in range(bx):
            c = ref[p + 1, 8 : 8 + by, :]
            s = ref[p, 8 : 8 + by, :] + ref[p + 2, 8 : 8 + by, :]
            s = s + ref[p + 1, 7 : 7 + by, :] + ref[p + 1, 9 : 9 + by, :]
            s = s + jnp.where(lane == 0, roll(zl, -p, 1), roll(c, 1, 1))
            s = s + jnp.where(lane == bz - 1, roll(zr, bz - 1 - p, 1), roll(c, -1, 1))
            out.append(6.0 * c - s)
        return jnp.stack(out)

    offsets = [
        (dx, dy, dz)
        for dx in range(-kx, kx + 1) for dy in range(-ky, ky + 1) for dz in (-1, 0, 1)
        if (dx, dy, dz) != (0, 0, 0) and abs(dx) < nx and abs(dy) < ny and abs(dz) < nz
    ]

    def gather(c, do):
        for dx, dy, dz in offsets:
            def copy(dx=dx, dy=dy, dz=dz):
                i = ((dx + kx) * (2 * ky + 1) + dy + ky) * 3 + dz + 1
                return pltpu.make_async_remote_copy(
                    dsrc.at[c],
                    win.at[c, 1 - dz, pl.ds((kx - dx) * hx, hx), pl.ds((ky - dy) * hy, hy)],
                    dsend.at[c, i], drecv.at[c, i],
                    device_id=(gx + dx, gy + dy, gz + dz), device_id_type=MESH,
                )

            def there(s):
                x, y, z = gx + s * dx, gy + s * dy, gz + s * dz
                return (x >= 0) & (x < nx) & (y >= 0) & (y < ny) & (z >= 0) & (z < nz)

            if do == "start":
                @pl.when(there(1))
                def _():
                    copy().start()
            else:
                @pl.when(there(1))
                def _():
                    copy().wait_send()

                @pl.when(there(-1))
                def _():
                    copy().wait_recv()

    wx, wy = (2 * kx + 1) * hx, (2 * ky + 1) * hy
    ex = kx * hx
    ey = ky * hy
    q = bz // 4

    def dims(n0, n1, half):
        shape = (n1 - n0, wy, bz)
        x = lax.broadcasted_iota(jnp.int32, shape, 0) + n0
        y = lax.broadcasted_iota(jnp.int32, shape, 1)
        z = lax.broadcasted_iota(jnp.int32, shape, 2)
        x = x + (gx * hx - ex) // half
        y = y + gy * hy - ey
        z = z + gz * hz - q
        return (
            (x >= 0) & (x < nx * hx // half) & (y >= 0) & (y < ny * hy) & (z >= 0) & (z < nz * hz)
        )

    def beside(v, step):
        m = v[1:-1]
        s = v[:-2] + v[2:]
        s = s + roll(m, step, 1) + roll(m, -step, 1)
        return s + roll(m, step, 2) + roll(m, -step, 2)

    def twin(v, axis):
        even = lax.broadcasted_iota(jnp.int32, v.shape, axis) % 2 == 0
        return v + jnp.where(even, roll(v, -1, axis), roll(v, 1, axis))

    def coarse(c):
        a0, a1 = ex - REACH, ex + hx + REACH
        zi = lane_of((a1 - a0, wy, bz))
        d = jnp.where(zi < q, win[c, 0, a0:a1], jnp.where(zi < q + hz, win[c, 1, a0:a1], win[c, 2, a0:a1]))
        v = W * d
        defect = d[1:-1] - (6.0 * v[1:-1] - beside(v, 1))
        n = defect.shape[0] // 2
        defect = defect.reshape(n, 2, wy, bz)
        r = 0.5 * twin(twin(defect[:, 0] + defect[:, 1], 1), 2)
        b0 = (a0 + 1) // 2
        m2 = dims(b0, b0 + n, 2)
        r = jnp.where(m2, r, 0.0)
        e = W * r
        e = jnp.where(m2[1:-1], e[1:-1] + W * (r[1:-1] - (6.0 * e[1:-1] - beside(e, 2))), 0.0)
        r = r[2:-2]
        e = jnp.where(m2[2:-2], e[1:-1] + W * (r - (6.0 * e[1:-1] - beside(e, 2))), 0.0)
        k0 = (b0 + 2) * 2 - a0
        spread = jnp.stack([e, e], axis=1).reshape(2 * e.shape[0], wy, bz)
        d = d[k0 : k0 + spread.shape[0]]
        v = W * d + spread
        out = v[1:-1] + W * (d[1:-1] - (6.0 * v[1:-1] - beside(v, 1)))
        p0 = (b0 + 2) * 2 + 1
        return jnp.where(dims(p0, p0 + out.shape[0], 1), out, 0.0), p0

    li = lax.broadcasted_iota(jnp.int32, (bz, bz), 0)
    lj = lax.broadcasted_iota(jnp.int32, (bz, bz), 1)
    shrink = jnp.where(li // 2 == (lj - q + hz) % hz, 0.5, 0.0).astype(f32)
    grow = jnp.where(li == q + lj // 2, 1.0, 0.0).astype(f32)
    dot = functools.partial(jnp.dot, precision=lax.Precision.HIGHEST, preferred_element_type=f32)

    def cycle_and_image(c, r):
        k = 2 * c
        exchange(k, r)
        rref = fld.at[k]
        rzl, rzr = zrec[k, 0], zrec[k, 1]
        defect = r - W * operate(rref, rzl, rzr)
        defect = defect.reshape(hx, 2, by, bz)
        tmp[...] = defect[:, 0] + defect[:, 1]
        half = tmp[:, pl.ds(0, hy, stride=2), :] + tmp[:, pl.ds(1, hy, stride=2), :]
        d1 = dot(half.reshape(hx * hy, bz), shrink).reshape(hx, hy, bz)
        dsrc[c] = d1
        win[c, 1, ex : ex + hx, ey : ey + hy, :] = d1
        gather(c, "start")
        gather(c, "wait")
        e1, p0 = coarse(c)
        e1 = e1[ex - 1 - p0 : ex + hx + 1 - p0, ey - 4 : ey + hy + 4]
        n = hy + 8
        prol[:, pl.ds(0, n, stride=2), :] = e1
        prol[:, pl.ds(1, n, stride=2), :] = e1
        own = prol[1 : hx + 1, 8 : 8 + by, :]
        vzl = W * rzl + pack(own, q - 1, 2)
        vzr = W * rzr + pack(own, q + hz, 2)
        fine = dot(prol[...].reshape((hx + 2) * 2 * n, bz), grow).reshape(hx + 2, 2 * n, bz)
        v = rest[0]
        for i in range(bx + 2):
            v[i] = W * rref[i] + fine[1 + (i - 1) // 2]
        z = v[1 : bx + 1, 8 : 8 + by, :] + W * (r - operate(v, vzl, vzr))
        exchange(k + 1, z)
        return z, operate(fld.at[k + 1], zrec[k + 1, 0], zrec[k + 1, 1])

    z0, w = cycle_and_image(0, r0)
    u, aw = cycle_and_image(1, w)

    pairs = ((r0, z0), (z0, w), (r0, u), (w, u), (u, aw), (z0, aw))
    l1 = lane_of((1, bz))
    mine = jnp.zeros((1, bz), f32)
    for i, (a, b) in enumerate(pairs):
        s = jnp.sum(jnp.sum(jnp.sum(a * b, axis=0), axis=0, keepdims=True), axis=1, keepdims=True)
        mine = jnp.where(l1 == i, s, mine)
    sums[me] = mine

    def share(do):
        def step(i, carry):
            other = lax.rem(me + i, total)
            source = lax.rem(me + total - i, total)
            if do == "start":
                pltpu.make_async_remote_copy(
                    sums.at[me], sums.at[me], ssend.at[i], srecv.at[i],
                    device_id=coords(other), device_id_type=MESH,
                ).start()
            else:
                pltpu.make_async_remote_copy(
                    sums.at[me], sums.at[source], ssend.at[i], srecv.at[i],
                    device_id=coords(other), device_id_type=MESH,
                ).wait()
            return carry

        lax.fori_loop(1, total, step, 0)

    share("start")
    share("wait")
    tot = jnp.sum(sums[...], axis=0)

    def scalar(i):
        return jnp.sum(jnp.where(l1 == i, tot, 0.0), axis=1, keepdims=True)

    g0, d0, ru, wu, uv, zv = (scalar(i) for i in range(6))
    a = g0 / d0
    g1 = (g0 - a * d0) - a * ru + a * a * wu
    beta = g1 / g0
    zaz = d0 - a * (wu + zv) + a * a * uv
    cross = (d0 - a * wu) + (d0 - a * zv)
    b = g1 / (zaz + beta * cross + beta * beta * d0)
    for p in range(bx):
        d1 = (z0[p] - a * u[p]) + beta * z0[p]
        i1 = (w[p] - a * aw[p]) + beta * w[p]
        sol[p] = a * z0[p] + b * d1
        res[p] = (r0[p] - a * w[p]) - b * i1


def solution(mesh):
    ns = tuple(mesh.shape[a] for a in ("gx", "gy", "gz"))

    def local(density, x_faces, y_faces, z_faces):
        bx, by, bz = density.shape
        kx = min(-(-REACH // (bx // 2)), 10**6)
        ky = -(-REACH // (by // 2))
        hx, hy = bx // 2, by // 2
        vm = pl.BlockSpec(memory_space=pltpu.VMEM)
        total = ns[0] * ns[1] * ns[2]
        near = (2 * kx + 1) * (2 * ky + 1) * 3
        f32 = jnp.float32
        dma = pltpu.SemaphoreType.DMA
        return pl.pallas_call(
            functools.partial(kernel, ns, bx, by, bz, kx, ky),
            out_shape=(jax.ShapeDtypeStruct(density.shape, f32),) * 2,
            in_specs=[vm] * 4,
            out_specs=(vm, vm),
            scratch_shapes=[
                pltpu.VMEM((4, bx + 2, by + 16, bz), f32),
                pltpu.VMEM((4, 2, bx, bz), f32),
                pltpu.VMEM((4, 2, bx, bz), f32),
                pltpu.VMEM((4, 2, by, bz), f32),
                pltpu.VMEM((4, 2, by, bz), f32),
                pltpu.VMEM((hx, by, bz), f32),
                pltpu.VMEM((hx + 2, by + 16, bz), f32),
                pltpu.VMEM((2, hx, hy, bz), f32),
                pltpu.VMEM((2, 3, (2 * kx + 1) * hx, (2 * ky + 1) * hy, bz), f32),
                pltpu.VMEM((total, 1, bz), f32),
                dma((4, 6)),
                dma((4, 6)),
                dma((2, near)),
                dma((2, near)),
                dma((total,)),
                dma((total,)),
                pltpu.VMEM((bx + 2, by + 16, bz), f32),
            ],
            compiler_params=pltpu.CompilerParams(collective_id=0, has_side_effects=True),
        )(density, x_faces, y_faces, z_faces)

    return jax.shard_map(
        local,
        mesh=mesh,
        in_specs=(P("gx", "gy", "gz"), P(None, "gy", "gz"), P(None, "gx", "gz"), P(None, "gx", "gy")),
        out_specs=(P("gx", "gy", "gz"), P("gx", "gy", "gz")),
        check_vma=False,
    )
```

```python
import functools

import jax
import jax.numpy as jnp
from jax import lax
from jax.experimental import pallas as pl
from jax.experimental.pallas import tpu as pltpu
from jax.sharding import PartitionSpec as P

W = 1.0 / 9.0
COUPLING = 0.5
MESH = pl.DeviceIdType.MESH
REACH = 7


def lane_of(shape):
    return lax.broadcasted_iota(jnp.int32, shape, len(shape) - 1)


def roll(x, shift, axis):
    return pltpu.roll(x, shift % x.shape[axis], axis)


def kernel(
    ns, bx, by, bz, kx, ky,
    den, xf, yf, zf, sol, res,
    fld, ysrc, yrec, zsrc, zrec, tmp, prol, dsrc, win, sums,
    fsend, frecv, dsend, drecv, ssend, srecv,
    xyrec, pk, vfld, vpk, zfld, zpk,
):
    nx, ny, nz = ns
    gx, gy, gz = (lax.axis_index(a) for a in ("gx", "gy", "gz"))
    hx, hy, hz = bx // 2, by // 2, bz // 2
    me = (gx * ny + gy) * nz + gz
    total = nx * ny * nz
    f32 = jnp.float32

    fld[...] = jnp.zeros_like(fld)
    yrec[...] = jnp.zeros_like(yrec)
    zrec[...] = jnp.zeros_like(zrec)
    win[...] = jnp.zeros_like(win)
    xyrec[...] = jnp.zeros_like(xyrec)
    pk[...] = jnp.zeros_like(pk)

    barrier = pltpu.get_barrier_semaphore()

    def coords(flat):
        return (flat // (ny * nz), lax.rem(flat // nz, ny), lax.rem(flat, nz))

    def greet(step, c):
        other = lax.rem(me + step, total)
        pl.semaphore_signal(barrier, inc=1, device_id=coords(other), device_id_type=MESH)
        return c

    lax.fori_loop(1, total, greet, 0)

    lane = lane_of((by, bz))
    eye = lax.broadcasted_iota(jnp.int32, (by, by), 0) == lax.broadcasted_iota(jnp.int32, (by, by), 1)
    row = lax.broadcasted_iota(jnp.int32, (by, bz), 0)
    planes = []
    for p in range(bx):
        r = -COUPLING * den[p]
        if p == 0:
            r = r + jnp.where(gx == 0, xf[0], 0.0)
        if p == bx - 1:
            r = r + jnp.where(gx == nx - 1, xf[1], 0.0)
        r = r + jnp.where((row == 0) & (gy == 0), yf[0, p : p + 1, :], 0.0)
        r = r + jnp.where((row == by - 1) & (gy == ny - 1), yf[1, p : p + 1, :], 0.0)
        for side, (at, edge) in enumerate(((0, 0), (bz - 1, nz - 1))):
            col = jnp.sum(jnp.where(eye, zf[side, p : p + 1, :], 0.0), axis=1, keepdims=True)
            r = r + jnp.where((lane == at) & (gz == edge), col, 0.0)
        planes.append(r)
    r0 = jnp.stack(planes)

    pl.semaphore_wait(barrier, total - 1)

    lane8 = lane_of((8, bz))
    lanef = lane_of((by + 16, bz))
    halves = by // 8
    own = pl.ds(8, by)

    def exists(x, y, z):
        return (x >= 0) & (x < nx) & (y >= 0) & (y < ny) & (z >= 0) & (z < nz)

    def transfer(items, do):
        for (dx, dy, dz), src, dst, ss, rs in items:
            def copy(src=src, dst=dst, ss=ss, rs=rs, to=(gx + dx, gy + dy, gz + dz)):
                return pltpu.make_async_remote_copy(
                    src, dst, ss, rs, device_id=to, device_id_type=MESH
                )

            if do == "start":
                @pl.when(exists(gx + dx, gy + dy, gz + dz))
                def _():
                    copy().start()
            elif do == "sent":
                @pl.when(exists(gx + dx, gy + dy, gz + dz))
                def _():
                    copy().wait_send()
            else:
                @pl.when(exists(gx - dx, gy - dy, gz - dz))
                def _():
                    copy().wait_recv()

    def messages(c):
        f = fld.at[c]
        raw = [
            ((1, 0, 0), f.at[bx : bx + 2, own], f.at[0:2, own]),
            ((-1, 0, 0), f.at[2:4, own], f.at[bx + 2 : bx + 4, own]),
            ((0, 1, 0), ysrc.at[c, 1], yrec.at[c, 0]),
            ((0, -1, 0), ysrc.at[c, 0], yrec.at[c, 1]),
        ]
        for dz in (1, -1):
            src, side = zsrc.at[c, (dz + 1) // 2], (1 - dz) // 2
            raw.append(((0, 0, dz), src, zrec.at[c, side, 0]))
            raw.append(((1, 0, dz), src, zrec.at[c, side, 1]))
            raw.append(((-1, 0, dz), src, zrec.at[c, side, 2]))
            raw.append(((0, 1, dz), src, zrec.at[c, side, 3]))
            raw.append(((0, -1, dz), src, zrec.at[c, side, 4]))
        for dx in (1, -1):
            for dy in (1, -1):
                i = (1 - dx) + (1 - dy) // 2
                raw.append(((dx, dy, 0), ysrc.at[c, (dy + 1) // 2, 0], xyrec.at[c, i]))
        return [
            (o, src, dst, fsend.at[c, i], frecv.at[c, i])
            for i, (o, src, dst) in enumerate(raw)
            if abs(o[0]) < nx and abs(o[1]) < ny and abs(o[2]) < nz
        ]

    def exchange(c, value):
        fld[c, 2 : bx + 2, 8 : 8 + by, :] = value
        for p in range(bx):
            for d in (0, 1):
                ysrc[c, 0, d, p : p + 1, :] = value[p, d : d + 1, :]
                ysrc[c, 1, d, p : p + 1, :] = value[p, by - 1 - d : by - d, :]
        for side, at in ((0, 0), (1, bz - 2)):
            out = jnp.zeros((8, bz), f32)
            for h in range(halves):
                for p in range(bx):
                    to = 2 * (h * bx + p)
                    moved = roll(value[p, 8 * h : 8 * h + 8, :], to - at, 1)
                    out = jnp.where(lane8 // 2 == to // 2, moved, out)
            zsrc[c, side] = out
        items = messages(c)
        transfer(items, "start")
        transfer(items, "here")
        for p in range(bx):
            for d in (0, 1):
                fld[c, p + 2, 7 - d : 8 - d, :] = yrec[c, 0, d, p : p + 1, :]
                fld[c, p + 2, 8 + by + d : 9 + by + d, :] = yrec[c, 1, d, p : p + 1, :]
        for i in range(4):
            plane, p = ((1, bx - 1), (bx + 2, 0))[i // 2]
            at = (7, 8 + by)[i % 2]
            fld[c, plane, at : at + 1, :] = xyrec[c, i, p : p + 1, :]
        for side in (0, 1):
            t = [zrec[c, side, i] for i in range(5)]
            for h in range(halves):
                o = jnp.where((lane8 >= 4) & (lane8 < 4 + 2 * bx), roll(t[0], 4 - 2 * bx * h, 1), 0.0)
                o = jnp.where(lane8 // 2 == 1, roll(t[1], 2 - 2 * (bx * h + bx - 1), 1), o)
                o = jnp.where(lane8 // 2 == bx + 2, roll(t[2], 2 * (bx + 2) - 2 * bx * h, 1), o)
                pk[c, side, 8 + 8 * h : 16 + 8 * h, :] = o
            inner = (lane8 >= 4) & (lane8 < 4 + 2 * bx)
            before = jnp.where(inner, roll(t[3], 4 - 2 * bx * (halves - 1), 1), 0.0)
            after = jnp.where(inner, roll(t[4], 4, 1), 0.0)
            pk[c, side, 7:8, :] = before[7:8]
            pk[c, side, 8 + by : 9 + by, :] = after[0:1]

    def operate(ref, packed, i, a, b):
        c = ref[i, a:b, :]
        ln = lane_of(c.shape)
        s = ref[i - 1, a:b, :] + ref[i + 1, a:b, :]
        s = s + ref[i, a - 1 : b - 1, :] + ref[i, a + 1 : b + 1, :]
        s = s + jnp.where(ln == 0, packed[0, a:b, 2 * i + 1 : 2 * i + 2], roll(c, 1, 1))
        s = s + jnp.where(ln == bz - 1, packed[1, a:b, 2 * i : 2 * i + 1], roll(c, -1, 1))
        return 6.0 * c - s

    offsets = [
        (dx, dy, dz)
        for dx in range(-kx, kx + 1) for dy in range(-ky, ky + 1) for dz in (-1, 0, 1)
        if (dx, dy, dz) != (0, 0, 0) and abs(dx) < nx and abs(dy) < ny and abs(dz) < nz
    ]

    def gathered(c):
        items = []
        for dx, dy, dz in offsets:
            i = ((dx + kx) * (2 * ky + 1) + dy + ky) * 3 + dz + 1
            dst = win.at[c, 1 - dz, pl.ds((kx - dx) * hx, hx), pl.ds((ky - dy) * hy, hy)]
            items.append(((dx, dy, dz), dsrc.at[c], dst, dsend.at[c, i], drecv.at[c, i]))
        return items

    wx, wy = (2 * kx + 1) * hx, (2 * ky + 1) * hy
    ex = kx * hx
    ey = ky * hy
    q = bz // 4

    def dims(n0, n1, half):
        shape = (n1 - n0, wy, bz)
        x = lax.broadcasted_iota(jnp.int32, shape, 0) + n0
        y = lax.broadcasted_iota(jnp.int32, shape, 1)
        z = lax.broadcasted_iota(jnp.int32, shape, 2)
        x = x + (gx * hx - ex) // half
        y = y + gy * hy - ey
        z = z + gz * hz - q
        return (
            (x >= 0) & (x < nx * hx // half) & (y >= 0) & (y < ny * hy) & (z >= 0) & (z < nz * hz)
        )

    def beside(v, step):
        m = v[1:-1]
        s = v[:-2] + v[2:]
        s = s + roll(m, step, 1) + roll(m, -step, 1)
        return s + roll(m, step, 2) + roll(m, -step, 2)

    def twin(v, axis):
        even = lax.broadcasted_iota(jnp.int32, v.shape, axis) % 2 == 0
        return v + jnp.where(even, roll(v, -1, axis), roll(v, 1, axis))

    def coarse(c):
        a0, a1 = ex - REACH, ex + hx + REACH
        zi = lane_of((a1 - a0, wy, bz))
        d = jnp.where(zi < q, win[c, 0, a0:a1], jnp.where(zi < q + hz, win[c, 1, a0:a1], win[c, 2, a0:a1]))
        v = W * d
        defect = d[1:-1] - (6.0 * v[1:-1] - beside(v, 1))
        n = defect.shape[0] // 2
        defect = defect.reshape(n, 2, wy, bz)
        r = 0.5 * twin(twin(defect[:, 0] + defect[:, 1], 1), 2)
        b0 = (a0 + 1) // 2
        m2 = dims(b0, b0 + n, 2)
        r = jnp.where(m2, r, 0.0)
        e = W * r
        e = jnp.where(m2[1:-1], e[1:-1] + W * (r[1:-1] - (6.0 * e[1:-1] - beside(e, 2))), 0.0)
        r = r[2:-2]
        e = jnp.where(m2[2:-2], e[1:-1] + W * (r - (6.0 * e[1:-1] - beside(e, 2))), 0.0)
        k0 = (b0 + 2) * 2 - a0
        spread = jnp.stack([e, e], axis=1).reshape(2 * e.shape[0], wy, bz)
        d = d[k0 : k0 + spread.shape[0]]
        v = W * d + spread
        out = v[1:-1] + W * (d[1:-1] - (6.0 * v[1:-1] - beside(v, 1)))
        p0 = (b0 + 2) * 2 + 1
        return jnp.where(dims(p0, p0 + out.shape[0], 1), out, 0.0), p0

    li = lax.broadcasted_iota(jnp.int32, (bz, bz), 0)
    lj = lax.broadcasted_iota(jnp.int32, (bz, bz), 1)
    shrink = jnp.where(li // 2 == (lj - q + hz) % hz, 0.5, 0.0).astype(f32)
    grow = jnp.where(li == q + lj // 2, 1.0, 0.0).astype(f32)
    dot = functools.partial(jnp.dot, precision=lax.Precision.HIGHEST, preferred_element_type=f32)

    def cycle_and_image(c, r):
        exchange(c, r)
        rref = fld.at[c]
        for j in range(hx):
            d = r[2 * j] + r[2 * j + 1]
            for i in (2 * j + 2, 2 * j + 3):
                d = d - W * operate(rref, pk.at[c], i, 8, 8 + by)
            tmp[j] = d
        half = tmp[:, pl.ds(0, hy, stride=2), :] + tmp[:, pl.ds(1, hy, stride=2), :]
        d1 = dot(half.reshape(hx * hy, bz), shrink).reshape(hx, hy, bz)
        dsrc[c] = d1
        win[c, 1, ex : ex + hx, ey : ey + hy, :] = d1
        transfer(gathered(c), "start")
        transfer(gathered(c), "here")
        e1, p0 = coarse(c)
        e1 = e1[ex - 1 - p0 : ex + hx + 1 - p0, ey - 4 : ey + hy + 4]
        n = hy + 8
        prol[:, pl.ds(0, n, stride=2), :] = e1
        prol[:, pl.ds(1, n, stride=2), :] = e1
        for side, at in ((0, q - 1), (1, q + hz)):
            o = W * pk[c, side]
            for j in range(hx + 2):
                o = o + jnp.where(lanef // 4 == j, prol[j, :, at : at + 1], 0.0)
            vpk[side] = o
        fine = dot(prol[...].reshape((hx + 2) * 2 * n, bz), grow).reshape(hx + 2, 2 * n, bz)
        for i in range(bx + 4):
            vfld[i] = W * rref[i] + fine[i // 2]
        for i in range(1, bx + 3):
            a, b = 7, 9 + by
            z = vfld[i, a:b, :] + W * (rref[i, a:b, :] - operate(vfld, vpk, i, a, b))
            zrow = lax.broadcasted_iota(jnp.int32, z.shape, 0)
            inside = ((zrow > 0) | (gy > 0)) & ((zrow < by + 1) | (gy < ny - 1))
            if i == 1:
                inside = inside & (gx > 0)
            if i == bx + 2:
                inside = inside & (gx < nx - 1)
            zfld[i, a:b, :] = jnp.where(inside, z, 0.0)
        for side, at in ((0, 0), (1, bz - 1)):
            o = vpk[side]
            s = roll(o, 2, 1) + roll(o, -2, 1) + roll(o, 1, 0) + roll(o, -1, 0)
            s = s + roll(o, 1 - 2 * side, 1)
            for i in range(2, bx + 2):
                s = s + jnp.where(lanef == 2 * i + 1 - side, vfld[i, :, at : at + 1], 0.0)
            inside = gz < nz - 1 if side else gz > 0
            zpk[side] = jnp.where(inside, o + W * (pk[c, side] - (6.0 * o - s)), 0.0)
        z = zfld[2 : bx + 2, 8 : 8 + by, :]
        return z, jnp.stack([operate(zfld, zpk, i, 8, 8 + by) for i in range(2, bx + 2)])

    z0, w = cycle_and_image(0, r0)
    u, aw = cycle_and_image(1, w)

    pairs = ((r0, z0), (z0, w), (r0, u), (w, u), (u, aw), (z0, aw))
    l1 = lane_of((1, bz))
    mine = jnp.zeros((1, bz), f32)
    for i, (a, b) in enumerate(pairs):
        s = jnp.sum(jnp.sum(jnp.sum(a * b, axis=0), axis=0, keepdims=True), axis=1, keepdims=True)
        mine = jnp.where(l1 == i, s, mine)
    sums[me] = mine

    def share(do):
        def step(i, carry):
            other = lax.rem(me + i, total)
            source = lax.rem(me + total - i, total)
            if do == "start":
                pltpu.make_async_remote_copy(
                    sums.at[me], sums.at[me], ssend.at[i], srecv.at[i],
                    device_id=coords(other), device_id_type=MESH,
                ).start()
            else:
                pltpu.make_async_remote_copy(
                    sums.at[me], sums.at[source], ssend.at[i], srecv.at[i],
                    device_id=coords(other), device_id_type=MESH,
                ).wait()
            return carry

        lax.fori_loop(1, total, step, 0)

    share("start")
    for c in (0, 1):
        transfer(messages(c), "sent")
        transfer(gathered(c), "sent")
    share("wait")
    tot = jnp.sum(sums[...], axis=0)

    def scalar(i):
        return jnp.sum(jnp.where(l1 == i, tot, 0.0), axis=1, keepdims=True)

    g0, d0, ru, wu, uv, zv = (scalar(i) for i in range(6))
    a = g0 / d0
    g1 = (g0 - a * d0) - a * ru + a * a * wu
    beta = g1 / g0
    zaz = d0 - a * (wu + zv) + a * a * uv
    cross = (d0 - a * wu) + (d0 - a * zv)
    b = g1 / (zaz + beta * cross + beta * beta * d0)
    for p in range(bx):
        d1 = (z0[p] - a * u[p]) + beta * z0[p]
        i1 = (w[p] - a * aw[p]) + beta * w[p]
        sol[p] = a * z0[p] + b * d1
        res[p] = (r0[p] - a * w[p]) - b * i1


def solution(mesh):
    ns = tuple(mesh.shape[a] for a in ("gx", "gy", "gz"))

    def local(density, x_faces, y_faces, z_faces):
        bx, by, bz = density.shape
        kx = min(-(-REACH // (bx // 2)), 10**6)
        ky = -(-REACH // (by // 2))
        hx, hy = bx // 2, by // 2
        vm = pl.BlockSpec(memory_space=pltpu.VMEM)
        total = ns[0] * ns[1] * ns[2]
        near = (2 * kx + 1) * (2 * ky + 1) * 3
        f32 = jnp.float32
        dma = pltpu.SemaphoreType.DMA
        return pl.pallas_call(
            functools.partial(kernel, ns, bx, by, bz, kx, ky),
            out_shape=(jax.ShapeDtypeStruct(density.shape, f32),) * 2,
            in_specs=[vm] * 4,
            out_specs=(vm, vm),
            scratch_shapes=[
                pltpu.VMEM((2, bx + 4, by + 16, bz), f32),
                pltpu.VMEM((2, 2, 2, bx, bz), f32),
                pltpu.VMEM((2, 2, 2, bx, bz), f32),
                pltpu.VMEM((2, 2, 8, bz), f32),
                pltpu.VMEM((2, 2, 5, 8, bz), f32),
                pltpu.VMEM((hx, by, bz), f32),
                pltpu.VMEM((hx + 2, by + 16, bz), f32),
                pltpu.VMEM((2, hx, hy, bz), f32),
                pltpu.VMEM((2, 3, (2 * kx + 1) * hx, (2 * ky + 1) * hy, bz), f32),
                pltpu.VMEM((total, 1, bz), f32),
                dma((2, 18)),
                dma((2, 18)),
                dma((2, near)),
                dma((2, near)),
                dma((total,)),
                dma((total,)),
                pltpu.VMEM((2, 4, bx, bz), f32),
                pltpu.VMEM((2, 2, by + 16, bz), f32),
                pltpu.VMEM((bx + 4, by + 16, bz), f32),
                pltpu.VMEM((2, by + 16, bz), f32),
                pltpu.VMEM((bx + 4, by + 16, bz), f32),
                pltpu.VMEM((2, by + 16, bz), f32),
            ],
            compiler_params=pltpu.CompilerParams(collective_id=0, has_side_effects=True),
        )(density, x_faces, y_faces, z_faces)

    return jax.shard_map(
        local,
        mesh=mesh,
        in_specs=(P("gx", "gy", "gz"), P(None, "gy", "gz"), P(None, "gx", "gz"), P(None, "gx", "gy")),
        out_specs=(P("gx", "gy", "gz"), P("gx", "gy", "gz")),
        check_vma=False,
    )
```

```python
import functools

import jax
import jax.numpy as jnp
from jax import lax
from jax.experimental import pallas as pl
from jax.experimental.pallas import tpu as pltpu
from jax.sharding import PartitionSpec as P

W = 1.0 / 9.0
COUPLING = 0.5
MESH = pl.DeviceIdType.MESH
REACH = 7


def lane_of(shape):
    return lax.broadcasted_iota(jnp.int32, shape, len(shape) - 1)


def roll(x, shift, axis):
    return pltpu.roll(x, shift % x.shape[axis], axis)


def kernel(
    ns, bx, by, bz, kx, ky,
    den_in, xf_in, yf_in, zf_in, sol, res,
    fld, ysrc, yrec, zsrc, zrec, tmp, prol, dsrc, dside, win, wside, sums,
    fsend, frecv, dsend, drecv, ssend, srecv,
    xyrec, pk, vfld, vpk, zfld, zpk, den, xf, yf, zf, isem,
):
    nx, ny, nz = ns
    gx, gy, gz = (lax.axis_index(a) for a in ("gx", "gy", "gz"))
    hx, hy, hz = bx // 2, by // 2, bz // 2
    me = (gx * ny + gy) * nz + gz
    total = nx * ny * nz
    f32 = jnp.float32

    loads = [
        pltpu.make_async_copy(a, b, isem.at[i])
        for i, (a, b) in enumerate(((den_in, den), (xf_in, xf), (yf_in, yf), (zf_in, zf)))
    ]
    for load in loads:
        load.start()

    fld[...] = jnp.zeros_like(fld)
    yrec[...] = jnp.zeros_like(yrec)
    zrec[...] = jnp.zeros_like(zrec)
    win[...] = jnp.zeros_like(win)
    wside[...] = jnp.zeros_like(wside)
    xyrec[...] = jnp.zeros_like(xyrec)
    pk[...] = jnp.zeros_like(pk)

    barrier = pltpu.get_barrier_semaphore()

    def coords(flat):
        return (flat // (ny * nz), lax.rem(flat // nz, ny), lax.rem(flat, nz))

    def greet(step, c):
        other = lax.rem(me + step, total)
        pl.semaphore_signal(barrier, inc=1, device_id=coords(other), device_id_type=MESH)
        return c

    lax.fori_loop(1, total, greet, 0)

    for load in loads:
        load.wait()

    lane = lane_of((by, bz))
    eye = lax.broadcasted_iota(jnp.int32, (by, by), 0) == lax.broadcasted_iota(jnp.int32, (by, by), 1)
    row = lax.broadcasted_iota(jnp.int32, (by, bz), 0)
    planes = []
    for p in range(bx):
        r = -COUPLING * den[p]
        if p == 0:
            r = r + jnp.where(gx == 0, xf[0], 0.0)
        if p == bx - 1:
            r = r + jnp.where(gx == nx - 1, xf[1], 0.0)
        r = r + jnp.where((row == 0) & (gy == 0), yf[0, p : p + 1, :], 0.0)
        r = r + jnp.where((row == by - 1) & (gy == ny - 1), yf[1, p : p + 1, :], 0.0)
        for side, (at, edge) in enumerate(((0, 0), (bz - 1, nz - 1))):
            col = jnp.sum(jnp.where(eye, zf[side, p : p + 1, :], 0.0), axis=1, keepdims=True)
            r = r + jnp.where((lane == at) & (gz == edge), col, 0.0)
        planes.append(r)
    r0 = jnp.stack(planes)

    lane8 = lane_of((8, bz))
    lanef = lane_of((by + 16, bz))
    halves = by // 8
    own = pl.ds(8, by)

    def exists(x, y, z):
        return (x >= 0) & (x < nx) & (y >= 0) & (y < ny) & (z >= 0) & (z < nz)

    def transfer(items, do):
        for (dx, dy, dz), src, dst, ss, rs in items:
            def copy(src=src, dst=dst, ss=ss, rs=rs, to=(gx + dx, gy + dy, gz + dz)):
                return pltpu.make_async_remote_copy(
                    src, dst, ss, rs, device_id=to, device_id_type=MESH
                )

            if do == "start":
                @pl.when(exists(gx + dx, gy + dy, gz + dz))
                def _():
                    copy().start()
            elif do == "sent":
                @pl.when(exists(gx + dx, gy + dy, gz + dz))
                def _():
                    copy().wait_send()
            else:
                @pl.when(exists(gx - dx, gy - dy, gz - dz))
                def _():
                    copy().wait_recv()

    def messages(c):
        f = fld.at[c]
        raw = [
            ((1, 0, 0), f.at[bx : bx + 2, own], f.at[0:2, own]),
            ((-1, 0, 0), f.at[2:4, own], f.at[bx + 2 : bx + 4, own]),
            ((0, 1, 0), ysrc.at[c, 1], yrec.at[c, 0]),
            ((0, -1, 0), ysrc.at[c, 0], yrec.at[c, 1]),
        ]
        for dz in (1, -1):
            src, side = zsrc.at[c, (dz + 1) // 2], (1 - dz) // 2
            raw.append(((0, 0, dz), src, zrec.at[c, side, 0]))
            raw.append(((1, 0, dz), src, zrec.at[c, side, 1]))
            raw.append(((-1, 0, dz), src, zrec.at[c, side, 2]))
            raw.append(((0, 1, dz), src, zrec.at[c, side, 3]))
            raw.append(((0, -1, dz), src, zrec.at[c, side, 4]))
        for dx in (1, -1):
            for dy in (1, -1):
                i = (1 - dx) + (1 - dy) // 2
                raw.append(((dx, dy, 0), ysrc.at[c, (dy + 1) // 2, 0], xyrec.at[c, i]))
        return [
            (o, src, dst, fsend.at[c, i], frecv.at[c, i])
            for i, (o, src, dst) in enumerate(raw)
            if abs(o[0]) < nx and abs(o[1]) < ny and abs(o[2]) < nz
        ]

    def exchange(c, value):
        fld[c, 2 : bx + 2, 8 : 8 + by, :] = value
        for p in range(bx):
            for d in (0, 1):
                ysrc[c, 0, d, p : p + 1, :] = value[p, d : d + 1, :]
                ysrc[c, 1, d, p : p + 1, :] = value[p, by - 1 - d : by - d, :]
        for side, at in ((0, 0), (1, bz - 2)):
            out = jnp.zeros((8, bz), f32)
            for h in range(halves):
                for p in range(bx):
                    to = 2 * (h * bx + p)
                    moved = roll(value[p, 8 * h : 8 * h + 8, :], to - at, 1)
                    out = jnp.where(lane8 // 2 == to // 2, moved, out)
            zsrc[c, side] = out
        items = messages(c)
        if c == 0:
            pl.semaphore_wait(barrier, total - 1)
        transfer(items, "start")
        transfer(items, "here")
        for p in range(bx):
            for d in (0, 1):
                fld[c, p + 2, 7 - d : 8 - d, :] = yrec[c, 0, d, p : p + 1, :]
                fld[c, p + 2, 8 + by + d : 9 + by + d, :] = yrec[c, 1, d, p : p + 1, :]
        for i in range(4):
            plane, p = ((1, bx - 1), (bx + 2, 0))[i // 2]
            at = (7, 8 + by)[i % 2]
            fld[c, plane, at : at + 1, :] = xyrec[c, i, p : p + 1, :]
        for side in (0, 1):
            t = [zrec[c, side, i] for i in range(5)]
            for h in range(halves):
                o = jnp.where((lane8 >= 4) & (lane8 < 4 + 2 * bx), roll(t[0], 4 - 2 * bx * h, 1), 0.0)
                o = jnp.where(lane8 // 2 == 1, roll(t[1], 2 - 2 * (bx * h + bx - 1), 1), o)
                o = jnp.where(lane8 // 2 == bx + 2, roll(t[2], 2 * (bx + 2) - 2 * bx * h, 1), o)
                pk[c, side, 8 + 8 * h : 16 + 8 * h, :] = o
            inner = (lane8 >= 4) & (lane8 < 4 + 2 * bx)
            before = jnp.where(inner, roll(t[3], 4 - 2 * bx * (halves - 1), 1), 0.0)
            after = jnp.where(inner, roll(t[4], 4, 1), 0.0)
            pk[c, side, 7:8, :] = before[7:8]
            pk[c, side, 8 + by : 9 + by, :] = after[0:1]

    def operate(ref, packed, i, a, b):
        c = ref[i, a:b, :]
        ln = lane_of(c.shape)
        s = ref[i - 1, a:b, :] + ref[i + 1, a:b, :]
        s = s + ref[i, a - 1 : b - 1, :] + ref[i, a + 1 : b + 1, :]
        s = s + jnp.where(ln == 0, packed[0, a:b, 2 * i + 1 : 2 * i + 2], roll(c, 1, 1))
        s = s + jnp.where(ln == bz - 1, packed[1, a:b, 2 * i : 2 * i + 1], roll(c, -1, 1))
        return 6.0 * c - s

    offsets = [
        (dx, dy, dz)
        for dx in range(-kx, kx + 1) for dy in range(-ky, ky + 1) for dz in (-1, 0, 1)
        if (dx, dy, dz) != (0, 0, 0) and abs(dx) < nx and abs(dy) < ny and abs(dz) < nz
    ]

    def gathered(c):
        items = []
        for dx, dy, dz in offsets:
            i = ((dx + kx) * (2 * ky + 1) + dy + ky) * 3 + dz + 1
            rows = pl.ds((ky - dy) * hy, hy)
            if dz == 0:
                n = hx // 2
                src, dst = dsrc.at[c], win.at[c, pl.ds((kx - dx) * n, n), rows]
            else:
                n = hx // 4
                side = (1 - dz) // 2
                src, dst = dside.at[c, 1 - side], wside.at[c, side, pl.ds((kx - dx) * n, n), rows]
            items.append(((dx, dy, dz), src, dst, dsend.at[c, i], drecv.at[c, i]))
        return items

    wx, wy = (2 * kx + 1) * hx, (2 * ky + 1) * hy
    ex = kx * hx
    ey = ky * hy
    q = bz // 4

    def dims(n0, n1, half):
        shape = (n1 - n0, wy, bz)
        x = lax.broadcasted_iota(jnp.int32, shape, 0) + n0
        y = lax.broadcasted_iota(jnp.int32, shape, 1)
        z = lax.broadcasted_iota(jnp.int32, shape, 2)
        x = x + (gx * hx - ex) // half
        y = y + gy * hy - ey
        z = z + gz * hz - q
        return (
            (x >= 0) & (x < nx * hx // half) & (y >= 0) & (y < ny * hy) & (z >= 0) & (z < nz * hz)
        )

    def beside(v, step):
        m = v[1:-1]
        s = v[:-2] + v[2:]
        s = s + roll(m, step, 1) + roll(m, -step, 1)
        return s + roll(m, step, 2) + roll(m, -step, 2)

    def twin(v, axis):
        even = lax.broadcasted_iota(jnp.int32, v.shape, axis) % 2 == 0
        return v + jnp.where(even, roll(v, -1, axis), roll(v, 1, axis))

    def coarse(c):
        a0, a1 = ex - REACH, ex + hx + REACH
        zi = lane_of((wy, bz))
        d = []
        for p in range(a0, a1):
            t, l, h = win[c, p // 2], wside[c, 0, p // 4], wside[c, 1, p // 4]
            t = roll(t, hz, 1) if p % 2 else t
            l = roll(l, -q * (p % 4), 1) if p % 4 else l
            h = roll(h, q + hz - q * (p % 4), 1) if p % 4 != 3 else h
            d.append(jnp.where(zi < q, l, jnp.where(zi < q + hz, t, h)))
        d = jnp.stack(d)
        v = W * d
        defect = d[1:-1] - (6.0 * v[1:-1] - beside(v, 1))
        n = defect.shape[0] // 2
        defect = defect.reshape(n, 2, wy, bz)
        r = 0.5 * twin(twin(defect[:, 0] + defect[:, 1], 1), 2)
        b0 = (a0 + 1) // 2
        m2 = dims(b0, b0 + n, 2)
        r = jnp.where(m2, r, 0.0)
        e = W * r
        e = jnp.where(m2[1:-1], e[1:-1] + W * (r[1:-1] - (6.0 * e[1:-1] - beside(e, 2))), 0.0)
        r = r[2:-2]
        e = jnp.where(m2[2:-2], e[1:-1] + W * (r - (6.0 * e[1:-1] - beside(e, 2))), 0.0)
        k0 = (b0 + 2) * 2 - a0
        spread = jnp.stack([e, e], axis=1).reshape(2 * e.shape[0], wy, bz)
        d = d[k0 : k0 + spread.shape[0]]
        v = W * d + spread
        out = v[1:-1] + W * (d[1:-1] - (6.0 * v[1:-1] - beside(v, 1)))
        p0 = (b0 + 2) * 2 + 1
        return jnp.where(dims(p0, p0 + out.shape[0], 1), out, 0.0), p0

    li = lax.broadcasted_iota(jnp.int32, (bz, bz), 0)
    lj = lax.broadcasted_iota(jnp.int32, (bz, bz), 1)
    shrink = jnp.where(li // 2 == (lj - q + hz) % hz, 0.5, 0.0).astype(f32)
    grow = jnp.where(li == q + lj // 2, 1.0, 0.0).astype(f32)

    def dot(x, m):
        out = None
        for _ in range(3):
            part = x.astype(jnp.bfloat16)
            x = x - part.astype(f32)
            y = jnp.dot(part, m.astype(jnp.bfloat16), preferred_element_type=f32)
            out = y if out is None else out + y
        return out

    def cycle_and_image(c, r):
        exchange(c, r)
        rref = fld.at[c]
        for j in range(hx):
            d = r[2 * j] + r[2 * j + 1]
            for i in (2 * j + 2, 2 * j + 3):
                d = d - W * operate(rref, pk.at[c], i, 8, 8 + by)
            tmp[j] = d
        half = tmp[:, pl.ds(0, hy, stride=2), :] + tmp[:, pl.ds(1, hy, stride=2), :]
        d1 = dot(half.reshape(hx * hy, bz), shrink).reshape(hx, hy, bz)
        li = lane_of((hy, bz))
        for j in range(hx // 2):
            t = jnp.where((li >= q) & (li < q + hz), d1[2 * j], d1[2 * j + 1])
            dsrc[c, j] = t
            win[c, ex // 2 + j, ey : ey + hy, :] = t
        for j in range(hx // 4):
            lo, hi = d1[4 * j], d1[4 * j]
            lo = roll(lo, q, 1)
            for m in range(1, 4):
                lo = jnp.where(li // q == m, roll(d1[4 * j + m], q * (m + 1), 1), lo)
                hi = jnp.where(li // q == m, roll(d1[4 * j + m], q * m, 1), hi)
            dside[c, 0, j] = lo
            dside[c, 1, j] = hi
        transfer(gathered(c), "start")
        transfer(gathered(c), "here")
        e1, p0 = coarse(c)
        e1 = e1[ex - 1 - p0 : ex + hx + 1 - p0, ey - 4 : ey + hy + 4]
        n = hy + 8
        prol[:, pl.ds(0, n, stride=2), :] = e1
        prol[:, pl.ds(1, n, stride=2), :] = e1
        for side, at in ((0, q - 1), (1, q + hz)):
            o = W * pk[c, side]
            for j in range(hx + 2):
                o = o + jnp.where(lanef // 4 == j, prol[j, :, at : at + 1], 0.0)
            vpk[side] = o
        fine = dot(prol[...].reshape((hx + 2) * 2 * n, bz), grow).reshape(hx + 2, 2 * n, bz)
        for i in range(bx + 4):
            vfld[i] = W * rref[i] + fine[i // 2]
        for i in range(1, bx + 3):
            a, b = 7, 9 + by
            z = vfld[i, a:b, :] + W * (rref[i, a:b, :] - operate(vfld, vpk, i, a, b))
            zrow = lax.broadcasted_iota(jnp.int32, z.shape, 0)
            inside = ((zrow > 0) | (gy > 0)) & ((zrow < by + 1) | (gy < ny - 1))
            if i == 1:
                inside = inside & (gx > 0)
            if i == bx + 2:
                inside = inside & (gx < nx - 1)
            zfld[i, a:b, :] = jnp.where(inside, z, 0.0)
        for side, at in ((0, 0), (1, bz - 1)):
            o = vpk[side]
            s = roll(o, 2, 1) + roll(o, -2, 1) + roll(o, 1, 0) + roll(o, -1, 0)
            s = s + roll(o, 1 - 2 * side, 1)
            for i in range(2, bx + 2):
                s = s + jnp.where(lanef == 2 * i + 1 - side, vfld[i, :, at : at + 1], 0.0)
            inside = gz < nz - 1 if side else gz > 0
            zpk[side] = jnp.where(inside, o + W * (pk[c, side] - (6.0 * o - s)), 0.0)
        z = zfld[2 : bx + 2, 8 : 8 + by, :]
        return z, jnp.stack([operate(zfld, zpk, i, 8, 8 + by) for i in range(2, bx + 2)])

    z0, w = cycle_and_image(0, r0)
    u, aw = cycle_and_image(1, w)

    pairs = ((r0, z0), (z0, w), (r0, u), (w, u), (u, aw), (z0, aw))
    l1 = lane_of((1, bz))
    mine = jnp.zeros((1, bz), f32)
    for i, (a, b) in enumerate(pairs):
        s = jnp.sum(jnp.sum(jnp.sum(a * b, axis=0), axis=0, keepdims=True), axis=1, keepdims=True)
        mine = jnp.where(l1 == i, s, mine)
    sums[me] = mine

    def share(do):
        def step(i, carry):
            other = lax.rem(me + i, total)
            source = lax.rem(me + total - i, total)
            if do == "start":
                pltpu.make_async_remote_copy(
                    sums.at[me], sums.at[me], ssend.at[i], srecv.at[i],
                    device_id=coords(other), device_id_type=MESH,
                ).start()
            else:
                pltpu.make_async_remote_copy(
                    sums.at[me], sums.at[source], ssend.at[i], srecv.at[i],
                    device_id=coords(other), device_id_type=MESH,
                ).wait()
            return carry

        lax.fori_loop(1, total, step, 0)

    share("start")
    for c in (0, 1):
        transfer(messages(c), "sent")
        transfer(gathered(c), "sent")
    share("wait")
    tot = jnp.sum(sums[...], axis=0)

    def scalar(i):
        return jnp.sum(jnp.where(l1 == i, tot, 0.0), axis=1, keepdims=True)

    g0, d0, ru, wu, uv, zv = (scalar(i) for i in range(6))
    a = g0 / d0
    g1 = (g0 - a * d0) - a * ru + a * a * wu
    beta = g1 / g0
    zaz = d0 - a * (wu + zv) + a * a * uv
    cross = (d0 - a * wu) + (d0 - a * zv)
    b = g1 / (zaz + beta * cross + beta * beta * d0)
    for p in range(bx):
        d1 = (z0[p] - a * u[p]) + beta * z0[p]
        i1 = (w[p] - a * aw[p]) + beta * w[p]
        sol[p] = a * z0[p] + b * d1
        res[p] = (r0[p] - a * w[p]) - b * i1


def solution(mesh):
    ns = tuple(mesh.shape[a] for a in ("gx", "gy", "gz"))

    def local(density, x_faces, y_faces, z_faces):
        bx, by, bz = density.shape
        kx = min(-(-REACH // (bx // 2)), 10**6)
        ky = -(-REACH // (by // 2))
        hx, hy = bx // 2, by // 2
        vm = pl.BlockSpec(memory_space=pltpu.VMEM)
        total = ns[0] * ns[1] * ns[2]
        near = (2 * kx + 1) * (2 * ky + 1) * 3
        f32 = jnp.float32
        dma = pltpu.SemaphoreType.DMA
        return pl.pallas_call(
            functools.partial(kernel, ns, bx, by, bz, kx, ky),
            out_shape=(jax.ShapeDtypeStruct(density.shape, f32),) * 2,
            in_specs=[pl.BlockSpec(memory_space=pl.ANY)] * 4,
            out_specs=(vm, vm),
            scratch_shapes=[
                pltpu.VMEM((2, bx + 4, by + 16, bz), f32),
                pltpu.VMEM((2, 2, 2, bx, bz), f32),
                pltpu.VMEM((2, 2, 2, bx, bz), f32),
                pltpu.VMEM((2, 2, 8, bz), f32),
                pltpu.VMEM((2, 2, 5, 8, bz), f32),
                pltpu.VMEM((hx, by, bz), f32),
                pltpu.VMEM((hx + 2, by + 16, bz), f32),
                pltpu.VMEM((2, hx // 2, hy, bz), f32),
                pltpu.VMEM((2, 2, hx // 4, hy, bz), f32),
                pltpu.VMEM((2, (2 * kx + 1) * hx // 2, (2 * ky + 1) * hy, bz), f32),
                pltpu.VMEM((2, 2, (2 * kx + 1) * hx // 4, (2 * ky + 1) * hy, bz), f32),
                pltpu.VMEM((total, 1, bz), f32),
                dma((2, 18)),
                dma((2, 18)),
                dma((2, near)),
                dma((2, near)),
                dma((total,)),
                dma((total,)),
                pltpu.VMEM((2, 4, bx, bz), f32),
                pltpu.VMEM((2, 2, by + 16, bz), f32),
                pltpu.VMEM((bx + 4, by + 16, bz), f32),
                pltpu.VMEM((2, by + 16, bz), f32),
                pltpu.VMEM((bx + 4, by + 16, bz), f32),
                pltpu.VMEM((2, by + 16, bz), f32),
                pltpu.VMEM(density.shape, f32),
                pltpu.VMEM(x_faces.shape, f32),
                pltpu.VMEM(y_faces.shape, f32),
                pltpu.VMEM(z_faces.shape, f32),
                dma((4,)),
            ],
            compiler_params=pltpu.CompilerParams(collective_id=0, has_side_effects=True),
        )(density, x_faces, y_faces, z_faces)

    return jax.shard_map(
        local,
        mesh=mesh,
        in_specs=(P("gx", "gy", "gz"), P(None, "gy", "gz"), P(None, "gx", "gz"), P(None, "gx", "gy")),
        out_specs=(P("gx", "gy", "gz"), P("gx", "gy", "gz")),
        check_vma=False,
    )
```
